32 devices in a mesh: dp: 4 (over x, y), tp: 8 (over z, core).
Axes of the slice: x: 2, y: 2, z: 4, core: 2. Of those that a mesh axis runs over, the one named last changes fastest.
Arguments:
- x: bfloat16 [4096, 8192], P(('dp', 'tp')), parts along dimension 0
- w_gate: bfloat16 [8192, 28672], P(None, 'tp')
- w_up: bfloat16 [8192, 28672], P(None, 'tp')
- w_down: bfloat16 [28672, 8192], P('tp')
Outputs:
- output: bfloat16 [4096, 8192], P(('dp', 'tp')), parts along dimension 0
There are 4 independent parts. The reference program is written for one: setup_inputs(seed, part) draws one part's arguments, and reference() takes and returns one part's arrays. A program takes and returns all parts, laid end to end along the dimension named above; an argument that names none is the same for every part.
All inputs are finite; a program needn't handle non-finite values.
Results may differ from the reference program's by a relative error of at most 0.016.
Values are sent between devices in bfloat16 or wider.
A program may use at most 2 GiB of HBM per device.

```python
import jax
import jax.numpy as jnp

ROWS = 1024
D = 8192
FF = 28672


def setup_inputs(seed: int = 0, part: int = 0) -> dict:
    kx, kg, ku, kd = jax.random.split(jax.random.key(seed), 4)
    drawn = {
        "x": jax.random.normal(jax.random.fold_in(kx, part), (ROWS, D), jnp.float32),
        "w_gate": jax.random.normal(kg, (D, FF), jnp.float32) * D**-0.5,
        "w_up": jax.random.normal(ku, (D, FF), jnp.float32) * D**-0.5,
        "w_down": jax.random.normal(kd, (FF, D), jnp.float32) * FF**-0.5,
    }
    return {k: v.astype(jnp.bfloat16) for k, v in drawn.items()}


def reference(x, w_gate, w_up, w_down):
    gate = jnp.dot(x, w_gate, preferred_element_type=jnp.float32)
    up = jnp.dot(x, w_up, preferred_element_type=jnp.float32)
    hidden = (jax.nn.silu(gate) * up).astype(jnp.bfloat16)
    return jnp.dot(hidden, w_down, preferred_element_type=jnp.float32).astype(jnp.bfloat16)
```

```python
import functools

import jax
import jax.numpy as jnp
from jax import lax
from jax.experimental import pallas as pl
from jax.experimental.pallas import tpu as pltpu
from jax.sharding import PartitionSpec as P

MESH = pl.DeviceIdType.MESH
F32, BF16 = jnp.float32, jnp.bfloat16
PIECES = 8
RING = 3
COMPUTE = 88
LAST = 108
A, B, F, N = 0, 1, 2, 3
IA, IB, OB, IF, IN = 0, 1, 2, 3, 4


def info(t, gj):
    two = 2 * gj
    u = jnp.maximum(t - two, 0)
    span = gj + PIECES
    ph = u // span
    v = u % span
    w = jnp.maximum(v - 4, 0)
    early = t < two
    mid = jnp.logical_and(t >= two, t < two + 2 * span)
    mid_gu = jnp.logical_and(v >= 4, jnp.logical_or(w >= 16, w % 4 != 3))
    is_gu = jnp.logical_or(early, jnp.logical_and(mid, mid_gu))
    i = jnp.where(early, t // gj, 2 + ph)
    j = jnp.where(early, t % gj, jnp.where(w >= 16, w - 4, (w // 4) * 3 + w % 4))
    k = jnp.maximum(t - two - 2 * span, 0)
    st = jnp.where(mid, ph, 2 + k % 2)
    n = jnp.where(mid, jnp.where(v < 4, v, 4 + w // 4), k // 2)
    seq = jnp.where(mid, ph * PIECES + n, 2 * PIECES + k)
    return is_gu, i, j, st, n, seq


def kernel(x_ref, wg_ref, wu_ref, wd_ref, y_ref, xg, wbuf, h, acc, pbuf, sbuf, ybuf, wsem, lsem, ag_p, ag_q, s_q, s_f, s_g,
           p_rx, i_rx, p_tx, s_tx, y_tx, fr_p, f_in, f_out):
    rows, d = x_ref.shape
    hid = wg_ref.shape[1]
    gn = wbuf.shape[-1]
    dn = d // PIECES
    gj = hid // gn
    half = rows // 2

    me = lax.axis_index("tp")
    z, c = me // 2, me % 2
    side = z // 2
    m = (z + side) % 2
    zi = z + 1 - 2 * side
    zo = z - 1 + 2 * side
    partner = {"tp": 2 * z + 1 - c}
    inward = {"tp": 2 * zi + c}
    outward = {"tp": 2 * zo + c}
    end, inner = m == 0, m == 1

    def block(zz, i):
        s = zz // 2
        return jnp.where(i == 0, zz, jnp.where(i == 1, zz + 1 - 2 * (zz % 2), jnp.where(i == 2, 2 - s, 3 - 3 * s)))

    def p_slot(st):
        i = jnp.where(st == A, 0, jnp.where(st == B, 1, jnp.where(st == F, 2, 3)))
        return 2 * block(z, i) + jnp.where(st == F, 1, 0)

    def i_slot(zz, kind):
        i = (0, 1, 2, 3, 0)[kind]
        return 2 * block(zz, i) + (1, 1, 0, 1, 0)[kind]

    def signal(sem, dev):
        pl.semaphore_signal(sem, inc=1, device_id=dev, device_id_type=MESH)

    def remote(src, dst, send, recv, dev):
        return pltpu.make_async_remote_copy(
            src_ref=src, dst_ref=dst, send_sem=send, recv_sem=recv, device_id=dev, device_id_type=MESH
        )

    def loads(t):
        is_gu, _, j, _, n, _ = info(t, gj)
        slot = t % RING
        gc = pl.ds(pl.multiple_of(j * gn, gn), gn)
        gu = [
            pltpu.make_async_copy(wg_ref.at[:, gc], wbuf.at[slot, 0], wsem.at[slot, 0]),
            pltpu.make_async_copy(wu_ref.at[:, gc], wbuf.at[slot, 1], wsem.at[slot, 1]),
        ]
        dd = [
            pltpu.make_async_copy(
                wd_ref.at[:, pl.ds(pl.multiple_of(n * dn + q * gn, gn), gn)],
                wbuf.at[slot, q // 2, pl.ds((q % 2) * hid, hid), :],
                wsem.at[slot, q],
            )
            for q in range(4)
        ]
        return is_gu, gu, dd

    def load(t):
        is_gu, gu, dd = loads(t)

        @pl.when(is_gu)
        def _():
            for cp in gu:
                cp.start()

        @pl.when(jnp.logical_not(is_gu))
        def _():
            for cp in dd:
                cp.start()

    load(jnp.int32(0))
    load(jnp.int32(1))
    own = pltpu.make_async_copy(x_ref, xg.at[me], lsem)
    own.start()

    barrier = pltpu.get_barrier_semaphore()
    signal(barrier, partner)

    @pl.when(z > 0)
    def _():
        signal(barrier, {"tp": me - 2})

    @pl.when(z < 3)
    def _():
        signal(barrier, {"tp": me + 2})

    pl.semaphore_wait(barrier, 3 - jnp.where(m == 0, 1, 0))

    def part(hh):
        return pl.ds(hh * half, half)

    def own_copies(hh):
        src, dst = x_ref.at[part(hh)], xg.at[me, part(hh)]
        return (
            remote(src, dst, s_q.at[z, hh], ag_q.at[z, hh], partner),
            remote(src, dst, s_f.at[z, hh], ag_p.at[z, hh], {"tp": me + 2}),
            remote(src, dst, s_g.at[hh], ag_p.at[z, hh], {"tp": me - 2}),
        )

    def per_way(hh, act):
        q, f, g = own_copies(hh)
        act(q)

        @pl.when(z < 3)
        def _():
            act(f)

        @pl.when(z > 0)
        def _():
            act(g)

    for hh in range(2):
        per_way(hh, lambda cp: cp.start())

    def fwd(o, hh, dev):
        piece = xg.at[2 * o + c, part(hh)]
        return (
            remote(piece, piece, s_q.at[o, hh], ag_q.at[o, hh], partner),
            remote(piece, piece, s_f.at[o, hh], ag_p.at[o, hh], dev),
        )

    def relay(k, hh):
        for sgn in (-1, 1):
            o, nxt = z + sgn * k, z - sgn

            @pl.when(jnp.logical_and(o >= 0, o <= 3))
            def _():
                to_p, on = fwd(o, hh, {"tp": 2 * nxt + c})
                on.wait_recv()
                to_p.start()

                @pl.when(jnp.logical_and(nxt >= 0, nxt <= 3))
                def _():
                    on.start()

    def arrived(o):
        for hh in range(2):
            piece = xg.at[2 * o + 1 - c, part(hh)]
            remote(piece, piece, s_q.at[o, hh], ag_q.at[o, hh], partner).wait_recv()

    def forwarded(o):
        nxt = jnp.where(o > z, z - 1, z + 1)
        for hh in range(2):
            to_p, on = fwd(o, hh, {"tp": 2 * nxt + c})
            to_p.wait_send()

            @pl.when(jnp.logical_and(nxt >= 0, nxt <= 3))
            def _():
                on.wait_send()

    def gate_up(t, i, j):
        b = block(z, i)
        hs = jnp.where(i == 3, 1 - m, i)
        slot = t % RING
        lhs = xg[pl.ds(2 * b, 2)].reshape(2 * rows, d)
        g = jnp.dot(lhs, wbuf[slot, 0], preferred_element_type=F32)
        u = jnp.dot(lhs, wbuf[slot, 1], preferred_element_type=F32)
        v = ((g / (1.0 + jnp.exp(-g))) * u).astype(BF16)
        cols = pl.ds(pl.multiple_of(j * gn, gn), gn)
        h[hs, c, :, cols] = v[:rows]
        h[hs, 1 - c, :, cols] = v[rows:]

    def down(t, st, n, seq):
        slot = t % RING
        hs = jnp.where(st == B, 2, jnp.where(st == N, m, 1 - m))
        ps = seq % 4
        lhs = h[hs].reshape(2 * rows, hid)
        for q in range(4):
            o = jnp.dot(lhs, wbuf[slot, q // 2, (q % 2) * hid:(q % 2 + 1) * hid, :], preferred_element_type=F32)
            acc[st % 2, n, :, q * gn:(q + 1) * gn] = o[:rows]
            pbuf[ps, :, q * gn:(q + 1) * gn] = o[rows:].astype(BF16)

    def cols_of(n):
        return pl.ds(pl.multiple_of(n * dn, dn), dn)

    def to_partner(st, n, seq):
        ps = seq % 4
        return remote(pbuf.at[ps], xg.at[p_slot(st), :, cols_of(n)], p_tx.at[ps], p_rx.at[st, n], partner)

    def incoming(kind, n):
        ref = xg.at[i_slot(z, kind), :, cols_of(n)]
        return ref, remote(ref, ref, s_tx.at[0, 0], i_rx.at[kind, n], inward)

    def chain(way, n, kind):
        dev, zz = (inward, zi) if way == 0 else (outward, zo)
        k = n % 4
        return remote(
            sbuf.at[way, k], xg.at[i_slot(zz, kind), :, cols_of(n)], s_tx.at[way, k], i_rx.at[kind, n], dev
        )

    def both_cores(st, n):
        ref = xg.at[p_slot(st), :, cols_of(n)]
        remote(ref, ref, p_tx.at[0], p_rx.at[st, n], partner).wait_recv()
        return acc[st % 2, n] + ref[...].astype(F32)

    def plus(val, kind, n):
        ref, cp = incoming(kind, n)
        cp.wait_recv()
        return val + ref[...].astype(F32)

    def send_on(st, n, way, kind_in, kind_out, first, free):
        @pl.when(n == 0)
        def _():
            pl.semaphore_wait(free, 1)

        @pl.when(jnp.logical_or(n >= 4, not first))
        def _():
            chain(way, n, kind_out).wait_send()

        val = both_cores(st, n)
        if kind_in is not None:
            val = plus(val, kind_in, n)
        sbuf[way, n % 4] = val.astype(BF16)
        chain(way, n, kind_out).start()

    def y_copy(n):
        return pltpu.make_async_copy(ybuf.at[n % 2], y_ref.at[:, cols_of(n)], y_tx.at[n % 2])

    def finish(val, n):
        @pl.when(n >= 2)
        def _():
            y_copy(n).wait()

        ybuf[n % 2] = val.astype(BF16)
        y_copy(n).start()

    def at(t, start, every, who):
        x = jnp.maximum(t - start, 0)
        hit = jnp.logical_and(jnp.logical_and(t >= start, x < every * PIECES), x % every == 0)
        return x // every, jnp.logical_and(hit, who)

    def step(t, carry):
        @pl.when(t + 2 < COMPUTE)
        def _():
            load(t + 2)

        @pl.when(t == 0)
        def _():
            own.wait()
            arrived(z)

        for when, k, hh in ((11, 1, 0), (14, 1, 1), (24, 2, 0), (32, 2, 1), (42, 3, 0), (54, 3, 1)):
            @pl.when(t == when)
            def _():
                relay(k, hh)

        for when, i in ((14, 1), (32, 2), (54, 3)):
            @pl.when(t == when)
            def _():
                arrived(block(z, i))

        @pl.when(t == 16)
        def _():
            signal(fr_p.at[0], partner)

            @pl.when(inner)
            def _():
                signal(f_in.at[0], outward)

        @pl.when(t == 29)
        def _():
            forwarded(block(z, 1))
            signal(fr_p.at[1], partner)

            @pl.when(inner)
            def _():
                signal(f_in.at[1], outward)

        @pl.when(t == 51)
        def _():
            for hh in range(2):
                per_way(hh, lambda cp: cp.wait_send())
            forwarded(block(z, 2))

            @pl.when(inner)
            def _():
                signal(f_in.at[1], inward)

        @pl.when(t == 58)
        def _():
            @pl.when(inner)
            def _():
                signal(f_in.at[2], inward)

            @pl.when(end)
            def _():
                signal(f_out, inward)

        @pl.when(t == 72)
        def _():
            forwarded(block(z, 3))
            signal(fr_p.at[2], partner)

            @pl.when(inner)
            def _():
                signal(f_in.at[2], outward)

        @pl.when(t < COMPUTE)
        def _():
            is_gu, gu, dd = loads(t)
            _, i, j, st, n, seq = info(t, gj)

            @pl.when(is_gu)
            def _():
                for cp in gu:
                    cp.wait()
                gate_up(t, i, j)

            @pl.when(jnp.logical_not(is_gu))
            def _():
                for cp in dd:
                    cp.wait()

                @pl.when(seq >= 4)
                def _():
                    to_partner(st, n, seq).wait_send()

                down(t, st, n, seq)
                for q in range(3):
                    @pl.when(seq == q * PIECES)
                    def _():
                        pl.semaphore_wait(fr_p.at[q], 1)
                to_partner(st, n, seq).start()

        def event(start, every, who, act):
            n, hit = at(t, start, every, who)

            @pl.when(hit)
            def _():
                act(n)

        event(30, 3, end, lambda n: send_on(A, n, 0, None, IA, True, f_in.at[0]))

        def keep(n):
            acc[0, n] = plus(both_cores(A, n), IA, n)

        event(34, 3, inner, keep)
        event(52, 3, end, lambda n: send_on(B, n, 0, None, IB, False, f_in.at[1]))
        event(56, 3, inner, lambda n: send_on(B, n, 0, IB, OB, True, f_in.at[1]))
        event(60, 3, inner, lambda n: finish(plus(acc[0, n], OB, n), n))
        event(74, 2, end, lambda n: send_on(F, n, 0, None, IF, False, f_in.at[2]))
        event(78, 3, inner, lambda n: send_on(F, n, 0, IF, IN, False, f_in.at[2]))
        event(82, 3, inner, lambda n: send_on(N, n, 1, IN, IN, True, f_out))
        event(86, 3, end, lambda n: finish(plus(both_cores(N, n), IN, n), n))
        return carry

    lax.fori_loop(0, LAST, step, 0)

    for n in (4, 5, 6, 7):
        chain(0, n, IN).wait_send()

        @pl.when(inner)
        def _():
            chain(1, n, IN).wait_send()

        to_partner(N, n, n).wait_send()
    for n in (6, 7):
        y_copy(n).wait()


def mlp(x, w_gate, w_up, w_down, vmem=67043328):
    rows, d = x.shape
    hid = w_gate.shape[1]
    dn = d // PIECES
    gn = dn // 4
    dma, reg = pltpu.SemaphoreType.DMA, pltpu.SemaphoreType.REGULAR
    return pl.pallas_call(
        kernel,
        name="mlp",
        out_shape=jax.ShapeDtypeStruct((rows, d), BF16),
        in_specs=[pl.BlockSpec(memory_space=pl.ANY)] * 4,
        out_specs=pl.BlockSpec(memory_space=pl.ANY),
        scratch_shapes=[
            pltpu.VMEM((8, rows, d), BF16),
            pltpu.VMEM((RING, 2, d, gn), BF16),
            pltpu.VMEM((3, 2, rows, hid), BF16),
            pltpu.VMEM((2, PIECES, rows, dn), F32),
            pltpu.VMEM((4, rows, dn), BF16),
            pltpu.VMEM((2, 4, rows, dn), BF16),
            pltpu.VMEM((2, rows, dn), BF16),
            dma((RING, 4)),
            dma,
            dma((4, 2)),
            dma((4, 2)),
            dma((4, 2)),
            dma((4, 2)),
            dma((2,)),
            dma((4, PIECES)),
            dma((5, PIECES)),
            dma((4,)),
            dma((2, 4)),
            dma((2,)),
            reg((3,)),
            reg((3,)),
            reg,
        ],
        compiler_params=pltpu.CompilerParams(collective_id=0, has_side_effects=True, vmem_limit_bytes=vmem),
    )(x, w_gate, w_up, w_down)


def solution(mesh):
    return jax.shard_map(
        mlp,
        mesh=mesh,
        in_specs=(P(("dp", "tp"), None), P(None, "tp"), P(None, "tp"), P("tp", None)),
        out_specs=P(("dp", "tp"), None),
        check_vma=False,
    )
```

```python
import functools

import jax
import jax.numpy as jnp
from jax import lax
from jax.experimental import pallas as pl
from jax.experimental.pallas import tpu as pltpu
from jax.sharding import PartitionSpec as P

MESH = pl.DeviceIdType.MESH
F32, BF16 = jnp.float32, jnp.bfloat16
PIECES = 8
RING = 3
PARTS = 4
COMPUTE = 88
LAST = 102
A, B, F, N = 0, 1, 2, 3
IA, IB, OB, IF, IN = 0, 1, 2, 3, 4


def div(a, b):
    return lax.div(jnp.int32(a), jnp.int32(b))


def rem(a, b):
    return lax.rem(jnp.int32(a), jnp.int32(b))


def third(t):
    q = div(t * 171, 512)
    return q, t - 3 * q


def info(t, gj):
    two, span = 2 * gj, gj + PIECES
    late = jnp.where(t >= gj, 1, 0)
    ph = jnp.where(t >= two + span, 1, 0)
    v = t - two - span * ph
    k = t - two - 2 * span
    kk = rem(k, 2)
    early, tail = t < two, k >= 0
    is_gu = jnp.logical_or(early, jnp.logical_and(v >= PIECES, jnp.logical_not(tail)))
    i = jnp.where(early, late, 2 + ph)
    j = jnp.where(early, t - gj * late, v - PIECES)
    st = jnp.where(tail, 2 + kk, ph)
    n = jnp.where(tail, div(k, 2), v)
    return is_gu, i, j, st, n, jnp.where(tail, 2 * PIECES + k, PIECES * ph + n)


def kernel(x_ref, wg_ref, wu_ref, wd_ref, y_ref, xg, wbuf, h, acc, pbuf, sbuf, ybuf, wsem, lsem, ag_p, ag_q, s_q, s_f, s_g,
           p_rx, i_rx, p_tx, s_tx, y_tx, fr_p, f_in, f_out):
    rows, d = x_ref.shape
    hid = wg_ref.shape[1]
    gn = wbuf.shape[-1]
    dn = d // PIECES
    gj = hid // gn
    half = rows // 2

    me = lax.axis_index("tp")
    z, c = div(me, 2), rem(me, 2)
    side = div(z, 2)
    m = rem(z + side, 2)
    zi = z + 1 - 2 * side
    zo = z - 1 + 2 * side
    partner = {"tp": 2 * z + 1 - c}
    inward = {"tp": 2 * zi + c}
    outward = {"tp": 2 * zo + c}
    end, inner = m == 0, m == 1

    def block(zz, i):
        s = div(zz, 2)
        return jnp.where(i == 0, zz, jnp.where(i == 1, zz + 1 - 2 * rem(zz, 2), jnp.where(i == 2, 2 - s, 3 - 3 * s)))

    def p_slot(st):
        i = jnp.where(st == A, 0, jnp.where(st == B, 1, jnp.where(st == F, 2, 3)))
        return 2 * block(z, i) + jnp.where(st == F, 1, 0)

    def i_slot(zz, kind):
        i = (0, 1, 2, 3, 0)[kind]
        return 2 * block(zz, i) + (1, 1, 0, 1, 0)[kind]

    def signal(sem, dev):
        pl.semaphore_signal(sem, inc=1, device_id=dev, device_id_type=MESH)

    def remote(src, dst, send, recv, dev):
        return pltpu.make_async_remote_copy(
            src_ref=src, dst_ref=dst, send_sem=send, recv_sem=recv, device_id=dev, device_id_type=MESH
        )

    def loads(t):
        is_gu, _, j, _, n, _ = info(t, gj)
        slot = third(t)[1]
        gc = pl.ds(pl.multiple_of(j * gn, gn), gn)
        gu = [
            pltpu.make_async_copy(wg_ref.at[:, gc], wbuf.at[slot, 0], wsem.at[slot, 0]),
            pltpu.make_async_copy(wu_ref.at[:, gc], wbuf.at[slot, 1], wsem.at[slot, 1]),
        ]
        dd = [
            pltpu.make_async_copy(
                wd_ref.at[:, pl.ds(pl.multiple_of(n * dn + q * gn, gn), gn)],
                wbuf.at[slot, q // 2, pl.ds((q % 2) * hid, hid), :],
                wsem.at[slot, q],
            )
            for q in range(4)
        ]
        return is_gu, gu, dd

    def load(t):
        is_gu, gu, dd = loads(t)

        @pl.when(is_gu)
        def _():
            for cp in gu:
                cp.start()

        @pl.when(jnp.logical_not(is_gu))
        def _():
            for cp in dd:
                cp.start()

    load(jnp.int32(0))
    load(jnp.int32(1))
    own = pltpu.make_async_copy(x_ref, xg.at[me], lsem)
    own.start()

    barrier = pltpu.get_barrier_semaphore()
    signal(barrier, partner)

    @pl.when(z > 0)
    def _():
        signal(barrier, {"tp": me - 2})

    @pl.when(z < 3)
    def _():
        signal(barrier, {"tp": me + 2})

    pl.semaphore_wait(barrier, 3 - jnp.where(m == 0, 1, 0))

    def part(hh):
        return pl.ds(hh * half, half)

    def own_copies(hh):
        src, dst = x_ref.at[part(hh)], xg.at[me, part(hh)]
        return (
            remote(src, dst, s_q.at[z, hh], ag_q.at[z, hh], partner),
            remote(src, dst, s_f.at[z, hh], ag_p.at[z, hh], {"tp": me + 2}),
            remote(src, dst, s_g.at[hh], ag_p.at[z, hh], {"tp": me - 2}),
        )

    def per_way(hh, act):
        q, f, g = own_copies(hh)
        act(q)

        @pl.when(z < 3)
        def _():
            act(f)

        @pl.when(z > 0)
        def _():
            act(g)

    for hh in range(2):
        per_way(hh, lambda cp: cp.start())

    def fwd(o, hh, dev):
        piece = xg.at[2 * o + c, part(hh)]
        return (
            remote(piece, piece, s_q.at[o, hh], ag_q.at[o, hh], partner),
            remote(piece, piece, s_f.at[o, hh], ag_p.at[o, hh], dev),
        )

    def relay(k, hh):
        for sgn in (-1, 1):
            o, nxt = z + sgn * k, z - sgn

            @pl.when(jnp.logical_and(o >= 0, o <= 3))
            def _():
                to_p, on = fwd(o, hh, {"tp": 2 * nxt + c})
                on.wait_recv()
                to_p.start()

                @pl.when(jnp.logical_and(nxt >= 0, nxt <= 3))
                def _():
                    on.start()

    def arrived(o):
        for hh in range(2):
            piece = xg.at[2 * o + 1 - c, part(hh)]
            remote(piece, piece, s_q.at[o, hh], ag_q.at[o, hh], partner).wait_recv()

    def forwarded(o):
        nxt = jnp.where(o > z, z - 1, z + 1)
        for hh in range(2):
            to_p, on = fwd(o, hh, {"tp": 2 * nxt + c})
            to_p.wait_send()

            @pl.when(jnp.logical_and(nxt >= 0, nxt <= 3))
            def _():
                on.wait_send()

    def gate_up(t, i, j):
        b = block(z, i)
        hs = jnp.where(i == 3, 1 - m, i)
        slot = third(t)[1]
        lhs = xg[pl.ds(2 * b, 2)].reshape(2 * rows, d)
        g = jnp.dot(lhs, wbuf[slot, 0], preferred_element_type=F32)
        u = jnp.dot(lhs, wbuf[slot, 1], preferred_element_type=F32)
        v = ((g / (1.0 + jnp.exp(-g))) * u).astype(BF16)
        cols = pl.ds(pl.multiple_of(j * gn, gn), gn)
        h[hs, c, :, cols] = v[:rows]
        h[hs, 1 - c, :, cols] = v[rows:]

    def down(t, st, n, seq):
        slot = third(t)[1]
        hs = jnp.where(st == B, 2, jnp.where(st == N, m, 1 - m))
        ps = rem(seq, 4)
        lhs = h[hs].reshape(2 * rows, hid)
        for q in range(4):
            o = jnp.dot(lhs, wbuf[slot, q // 2, (q % 2) * hid:(q % 2 + 1) * hid, :], preferred_element_type=F32)
            acc[rem(st, 2), n, :, q * gn:(q + 1) * gn] = o[:rows]
            pbuf[ps, :, q * gn:(q + 1) * gn] = o[rows:].astype(BF16)

    def cols_of(n):
        return pl.ds(pl.multiple_of(n * dn, dn), dn)

    def to_partner(st, n, seq):
        ps = rem(seq, 4)
        return remote(pbuf.at[ps], xg.at[p_slot(st), :, cols_of(n)], p_tx.at[ps], p_rx.at[st, n], partner)

    hc = dn // PARTS

    def half_of(n, e):
        return pl.ds(pl.multiple_of(n * dn + e * hc, hc), hc)

    def incoming(kind, n, e):
        ref = xg.at[i_slot(z, kind), :, half_of(n, e)]
        return ref, remote(ref, ref, s_tx.at[0, 0, 0], i_rx.at[kind, n, e], inward)

    def chain(way, n, e, kind):
        dev, zz = (inward, zi) if way == 0 else (outward, zo)
        k = rem(n, 4)
        return remote(
            sbuf.at[way, k, e], xg.at[i_slot(zz, kind), :, half_of(n, e)], s_tx.at[way, k, e], i_rx.at[kind, n, e], dev
        )

    def from_partner(st, n):
        ref = xg.at[p_slot(st), :, cols_of(n)]
        remote(ref, ref, p_tx.at[0], p_rx.at[st, n], partner).wait_recv()

    def both_cores(st, n, e):
        return acc[rem(st, 2), n, :, pl.ds(pl.multiple_of(e * hc, hc), hc)] + xg[p_slot(st), :, half_of(n, e)].astype(F32)

    def plus(val, kind, n, e):
        ref, cp = incoming(kind, n, e)
        cp.wait_recv()
        return val + ref[...].astype(F32)

    def ready(st, n, free):
        @pl.when(n == 0)
        def _():
            pl.semaphore_wait(free, 1)

        from_partner(st, n)

    def send_part(st, n, e, way, kind_in, kind_out, first):
        @pl.when(jnp.logical_or(n >= 4, not first))
        def _():
            chain(way, n, e, kind_out).wait_send()

        val = both_cores(st, n, e)
        if kind_in is not None:
            val = plus(val, kind_in, n, e)
        sbuf[way, rem(n, 4), e] = val.astype(BF16)
        chain(way, n, e, kind_out).start()

    def send_on(st, n, way, kind_in, kind_out, first, free):
        ready(st, n, free)
        for e in range(PARTS):
            send_part(st, n, e, way, kind_in, kind_out, first)

    def y_copy(n):
        k = rem(n, 2)
        return pltpu.make_async_copy(ybuf.at[k], y_ref.at[:, cols_of(n)], y_tx.at[k])

    def finish(val, n):
        @pl.when(n >= 2)
        def _():
            y_copy(n).wait()

        for e in range(PARTS):
            ybuf[rem(n, 2), :, e * hc:(e + 1) * hc] = val(e).astype(BF16)
        y_copy(n).start()

    def at(t, start, every, who):
        x = 2 * (t - start)
        n = div(x, 4) if every == 4 else div(x * 205, 1024)
        r = x - every * n
        hit = jnp.logical_and(jnp.logical_and(x >= 0, n < PIECES), r < 2)
        return n, jnp.logical_and(hit, who)

    def step(t, carry):
        @pl.when(t + 2 < COMPUTE)
        def _():
            load(t + 2)

        some = functools.reduce(jnp.logical_or, [t == w for w in (0, 13, 14, 16, 25, 34, 36, 44, 45, 51, 55, 58, 72)])

        @pl.when(some)
        def _():
            @pl.when(t == 0)
            def _():
                own.wait()
                arrived(z)

            for when, k, hh in ((13, 1, 0), (14, 1, 1), (25, 2, 0), (34, 2, 1), (45, 3, 0), (55, 3, 1)):
                @pl.when(t == when)
                def _():
                    relay(k, hh)

            for when, i in ((14, 1), (36, 2), (58, 3)):
                @pl.when(t == when)
                def _():
                    arrived(block(z, i))

            @pl.when(t == 16)
            def _():
                signal(fr_p.at[0], partner)

                @pl.when(inner)
                def _():
                    signal(f_in.at[0], outward)

            @pl.when(t == 44)
            def _():
                forwarded(block(z, 1))
                signal(fr_p.at[1], partner)

                @pl.when(inner)
                def _():
                    signal(f_in.at[1], outward)

            @pl.when(t == 51)
            def _():
                for hh in range(2):
                    per_way(hh, lambda cp: cp.wait_send())
                forwarded(block(z, 2))

                @pl.when(inner)
                def _():
                    signal(f_in.at[1], inward)

            @pl.when(t == 58)
            def _():
                @pl.when(inner)
                def _():
                    signal(f_in.at[2], inward)

                @pl.when(end)
                def _():
                    signal(f_out, inward)

            @pl.when(t == 72)
            def _():
                forwarded(block(z, 3))
                signal(fr_p.at[2], partner)

                @pl.when(inner)
                def _():
                    signal(f_in.at[2], outward)

        @pl.when(t < COMPUTE)
        def _():
            is_gu, gu, dd = loads(t)
            _, i, j, st, n, seq = info(t, gj)

            @pl.when(is_gu)
            def _():
                for cp in gu:
                    cp.wait()
                gate_up(t, i, j)

            @pl.when(jnp.logical_not(is_gu))
            def _():
                for cp in dd:
                    cp.wait()

                @pl.when(seq >= 4)
                def _():
                    to_partner(st, n, seq).wait_send()

                down(t, st, n, seq)
                for q in range(3):
                    @pl.when(seq == q * PIECES)
                    def _():
                        pl.semaphore_wait(fr_p.at[q], 1)
                to_partner(st, n, seq).start()

        def keep(n):
            from_partner(A, n)
            for e in range(PARTS):
                acc[0, n, :, e * hc:(e + 1) * hc] = plus(both_cores(A, n, e), IA, n, e)

        def last(n):
            from_partner(N, n)
            finish(lambda e: plus(both_cores(N, n, e), IN, n, e), n)

        def pieces():
            for b in range(2):
                for st, way, kind, free, g in (
                    (F, 0, IF, f_in.at[2], 2 * (t - 75) + b),
                    (N, 1, IN, f_out, 2 * (t - 75) + b - PARTS),
                ):
                    n, e = div(g, PARTS), rem(g, PARTS)

                    @pl.when(jnp.logical_and(g >= 0, g < PARTS * PIECES))
                    def _():
                        @pl.when(e == 0)
                        def _():
                            ready(st, n, free)

                        send_part(st, n, e, way, kind, IN, st == N)

        def event(start, every, who, act):
            n, hit = at(t, start, every, who)

            @pl.when(hit)
            def _():
                act(n)

        @pl.when(jnp.logical_and(t >= 30, t < 56))
        def _():
            event(30, 4, end, lambda n: send_on(A, n, 0, None, IA, True, f_in.at[0]))
            event(34, 5, inner, keep)

        @pl.when(jnp.logical_and(t >= 52, t < 80))
        def _():
            event(52, 4, end, lambda n: send_on(B, n, 0, None, IB, False, f_in.at[1]))
            event(56, 5, inner, lambda n: send_on(B, n, 0, IB, OB, True, f_in.at[1]))
            event(60, 5, inner, lambda n: finish(lambda e: plus(acc[0, n, :, e * hc:(e + 1) * hc], OB, n, e), n))

        @pl.when(t >= 73)
        def _():
            event(73, 4, end, lambda n: send_on(F, n, 0, None, IF, False, f_in.at[2]))
            event(83, 5, end, last)

            @pl.when(jnp.logical_and(t >= 75, inner))
            def _():
                pieces()

        return carry

    lax.fori_loop(0, LAST, step, 0)

    for n in (4, 5, 6, 7):
        for e in range(PARTS):
            chain(0, n, e, IN).wait_send()

        @pl.when(inner)
        def _():
            for e in range(PARTS):
                chain(1, n, e, IN).wait_send()

        to_partner(N, n, n).wait_send()
    for n in (6, 7):
        y_copy(n).wait()


def mlp(x, w_gate, w_up, w_down, vmem=67043328):
    rows, d = x.shape
    hid = w_gate.shape[1]
    dn = d // PIECES
    gn = dn // 4
    dma, reg = pltpu.SemaphoreType.DMA, pltpu.SemaphoreType.REGULAR
    return pl.pallas_call(
        kernel,
        name="mlp",
        out_shape=jax.ShapeDtypeStruct((rows, d), BF16),
        in_specs=[pl.BlockSpec(memory_space=pl.ANY)] * 4,
        out_specs=pl.BlockSpec(memory_space=pl.ANY),
        scratch_shapes=[
            pltpu.VMEM((8, rows, d), BF16),
            pltpu.VMEM((RING, 2, d, gn), BF16),
            pltpu.VMEM((3, 2, rows, hid), BF16),
            pltpu.VMEM((2, PIECES, rows, dn), F32),
            pltpu.VMEM((4, rows, dn), BF16),
            pltpu.VMEM((2, 4, PARTS, rows, dn // PARTS), BF16),
            pltpu.VMEM((2, rows, dn), BF16),
            dma((RING, 4)),
            dma,
            dma((4, 2)),
            dma((4, 2)),
            dma((4, 2)),
            dma((4, 2)),
            dma((2,)),
            dma((4, PIECES)),
            dma((5, PIECES, PARTS)),
            dma((4,)),
            dma((2, 4, PARTS)),
            dma((2,)),
            reg((3,)),
            reg((3,)),
            reg,
        ],
        compiler_params=pltpu.CompilerParams(collective_id=0, has_side_effects=True, vmem_limit_bytes=vmem),
    )(x, w_gate, w_up, w_down)


def solution(mesh):
    return jax.shard_map(
        mlp,
        mesh=mesh,
        in_specs=(P(("dp", "tp"), None), P(None, "tp"), P(None, "tp"), P("tp", None)),
        out_specs=P(("dp", "tp"), None),
        check_vma=False,
    )
```

```python
import functools

import jax
import jax.numpy as jnp
from jax import lax
from jax.experimental import pallas as pl
from jax.experimental.pallas import tpu as pltpu
from jax.sharding import PartitionSpec as P

MESH = pl.DeviceIdType.MESH
F32, BF16 = jnp.float32, jnp.bfloat16
PIECES = 8
RING = 3
PARTS = 4
COMPUTE = 88
LAST = 102
A, B, F, N = 0, 1, 2, 3
IA, IB, OB, IF, IN = 0, 1, 2, 3, 4


def div(a, b):
    return lax.div(jnp.int32(a), jnp.int32(b))


def rem(a, b):
    return lax.rem(jnp.int32(a), jnp.int32(b))


def third(t):
    return t - 3 * div(t * 171, 512)


def parity(st):
    return st % 2 if isinstance(st, int) else rem(st, 2)


def passes(gj):
    out, t = [], 0
    for gu, what in ((True, 0), (True, 1), (False, (A,)), (True, 2), (False, (B,)), (True, 3), (False, (F, N))):
        end = t + (gj if gu else PIECES * len(what))
        out.append((t, end, gu, what))
        t = end
    return out


def place(t, lo, what):
    k = t - lo
    if len(what) == 1:
        return what[0], k, PIECES * what[0] + k
    q = rem(k, 2)
    return what[0] + q, div(k, 2), PIECES * what[0] + k


def kernel(x_ref, wg_ref, wu_ref, wd_ref, y_ref, xg, wbuf, h, gs, us, acc, pbuf, sbuf, ybuf, wsem, lsem, ag_p, ag_q, s_q, s_f, s_g,
           p_rx, i_rx, p_tx, s_tx, y_tx, fr_p, f_in, f_out):
    rows, d = x_ref.shape
    hid = wg_ref.shape[1]
    gn = wbuf.shape[-1]
    dn = d // PIECES
    gj = hid // gn
    half = rows // 2

    me = lax.axis_index("tp")
    z, c = div(me, 2), rem(me, 2)
    side = div(z, 2)
    m = rem(z + side, 2)
    zi = z + 1 - 2 * side
    zo = z - 1 + 2 * side
    partner = {"tp": 2 * z + 1 - c}
    inward = {"tp": 2 * zi + c}
    outward = {"tp": 2 * zo + c}
    end, inner = m == 0, m == 1

    def block(zz, i):
        s = div(zz, 2)
        return (zz, zz + 1 - 2 * rem(zz, 2), 2 - s, 3 - 3 * s)[i]

    def p_slot(st):
        if isinstance(st, int):
            return 2 * block(z, st) + (1 if st == F else 0)
        return jnp.where(st == F, p_slot(F), p_slot(N))

    def i_slot(zz, kind):
        i = (0, 1, 2, 3, 0)[kind]
        return 2 * block(zz, i) + (1, 1, 0, 1, 0)[kind]

    def signal(sem, dev):
        pl.semaphore_signal(sem, inc=1, device_id=dev, device_id_type=MESH)

    def remote(src, dst, send, recv, dev):
        return pltpu.make_async_remote_copy(
            src_ref=src, dst_ref=dst, send_sem=send, recv_sem=recv, device_id=dev, device_id_type=MESH
        )

    segments = passes(gj)

    def copies(t, seg):
        lo, _, gu, what = seg
        slot = third(t)
        if gu:
            gc = pl.ds(pl.multiple_of((t - lo) * gn, gn), gn)
            return [
                pltpu.make_async_copy(wg_ref.at[:, gc], wbuf.at[slot, 0], wsem.at[slot, 0]),
                pltpu.make_async_copy(wu_ref.at[:, gc], wbuf.at[slot, 1], wsem.at[slot, 1]),
            ]
        _, n, _ = place(t, lo, what)
        return [
            pltpu.make_async_copy(
                wd_ref.at[:, pl.ds(pl.multiple_of(n * dn + q * gn, gn), gn)],
                wbuf.at[slot, q // 2, pl.ds((q % 2) * hid, hid), :],
                wsem.at[slot, q],
            )
            for q in range(4)
        ]

    def load(t, seg):
        for cp in copies(t, seg):
            cp.start()

    load(jnp.int32(0), segments[0])
    load(jnp.int32(1), segments[0])
    own = pltpu.make_async_copy(x_ref, xg.at[me], lsem)
    own.start()

    barrier = pltpu.get_barrier_semaphore()
    signal(barrier, partner)

    @pl.when(z > 0)
    def _():
        signal(barrier, {"tp": me - 2})

    @pl.when(z < 3)
    def _():
        signal(barrier, {"tp": me + 2})

    pl.semaphore_wait(barrier, 3 - jnp.where(m == 0, 1, 0))

    def part(hh):
        return pl.ds(hh * half, half)

    def own_copies(hh):
        src, dst = x_ref.at[part(hh)], xg.at[me, part(hh)]
        return (
            remote(src, dst, s_q.at[z, hh], ag_q.at[z, hh], partner),
            remote(src, dst, s_f.at[z, hh], ag_p.at[z, hh], {"tp": me + 2}),
            remote(src, dst, s_g.at[hh], ag_p.at[z, hh], {"tp": me - 2}),
        )

    def per_way(hh, act):
        q, f, g = own_copies(hh)
        act(q)

        @pl.when(z < 3)
        def _():
            act(f)

        @pl.when(z > 0)
        def _():
            act(g)

    for hh in range(2):
        per_way(hh, lambda cp: cp.start())

    def fwd(o, hh, dev):
        piece = xg.at[2 * o + c, part(hh)]
        return (
            remote(piece, piece, s_q.at[o, hh], ag_q.at[o, hh], partner),
            remote(piece, piece, s_f.at[o, hh], ag_p.at[o, hh], dev),
        )

    def relay(k, hh):
        for sgn in (-1, 1):
            o, nxt = z + sgn * k, z - sgn

            @pl.when(jnp.logical_and(o >= 0, o <= 3))
            def _():
                to_p, on = fwd(o, hh, {"tp": 2 * nxt + c})
                on.wait_recv()
                to_p.start()

                @pl.when(jnp.logical_and(nxt >= 0, nxt <= 3))
                def _():
                    on.start()

    def arrived(o):
        for hh in range(2):
            piece = xg.at[2 * o + 1 - c, part(hh)]
            remote(piece, piece, s_q.at[o, hh], ag_q.at[o, hh], partner).wait_recv()

    def forwarded(o):
        nxt = jnp.where(o > z, z - 1, z + 1)
        for hh in range(2):
            to_p, on = fwd(o, hh, {"tp": 2 * nxt + c})
            to_p.wait_send()

            @pl.when(jnp.logical_and(nxt >= 0, nxt <= 3))
            def _():
                on.wait_send()

    def hidden(hs, j):
        g, u = gs[...], us[...]
        v = ((g / (1.0 + jnp.exp(-g))) * u).astype(BF16)
        cols = pl.ds(pl.multiple_of(j * gn, gn), gn)
        h[hs, c, :, cols] = v[:rows]
        h[hs, 1 - c, :, cols] = v[rows:]

    def gate_up(t, i, j):
        b = block(z, i)
        hs = 1 - m if i == 3 else i
        slot = third(t)
        hidden(hs, jnp.maximum(j - 1, 0))
        lhs = xg[pl.ds(2 * b, 2)].reshape(2 * rows, d)
        g = jnp.dot(lhs, wbuf[slot, 0], preferred_element_type=F32)
        u = jnp.dot(lhs, wbuf[slot, 1], preferred_element_type=F32)
        gs[...] = g
        us[...] = u

        @pl.when(j == gj - 1)
        def _():
            hidden(hs, j)

    def down(t, st, n, seq):
        slot = third(t)
        hs = (1 - m, 2)[st] if isinstance(st, int) else jnp.where(st == N, m, 1 - m)
        ps = rem(seq, 4)
        lhs = h[hs].reshape(2 * rows, hid)
        for q in range(4):
            o = jnp.dot(lhs, wbuf[slot, q // 2, (q % 2) * hid:(q % 2 + 1) * hid, :], preferred_element_type=F32)
            acc[parity(st), n, :, q * gn:(q + 1) * gn] = o[:rows]
            pbuf[ps, :, q * gn:(q + 1) * gn] = o[rows:].astype(BF16)

    def cols_of(n):
        return pl.ds(pl.multiple_of(n * dn, dn), dn)

    def to_partner(st, n, seq):
        ps = rem(seq, 4)
        return remote(pbuf.at[ps], xg.at[p_slot(st), :, cols_of(n)], p_tx.at[ps], p_rx.at[st, n], partner)

    hc = dn // PARTS

    def half_of(n, e):
        return pl.ds(pl.multiple_of(n * dn + e * hc, hc), hc)

    def incoming(kind, n, e):
        ref = xg.at[i_slot(z, kind), :, half_of(n, e)]
        return ref, remote(ref, ref, s_tx.at[0, 0, 0], i_rx.at[kind, n, e], inward)

    def chain(way, n, e, kind):
        dev, zz = (inward, zi) if way == 0 else (outward, zo)
        k = rem(n, 4)
        return remote(
            sbuf.at[way, k, e], xg.at[i_slot(zz, kind), :, half_of(n, e)], s_tx.at[way, k, e], i_rx.at[kind, n, e], dev
        )

    def from_partner(st, n):
        ref = xg.at[p_slot(st), :, cols_of(n)]
        remote(ref, ref, p_tx.at[0], p_rx.at[st, n], partner).wait_recv()

    def both_cores(st, n, e):
        return acc[parity(st), n, :, pl.ds(pl.multiple_of(e * hc, hc), hc)] + xg[p_slot(st), :, half_of(n, e)].astype(F32)

    def plus(val, kind, n, e):
        ref, cp = incoming(kind, n, e)
        cp.wait_recv()
        return val + ref[...].astype(F32)

    def ready(st, n, free):
        @pl.when(n == 0)
        def _():
            pl.semaphore_wait(free, 1)

        from_partner(st, n)

    def send_part(st, n, e, way, kind_in, kind_out, first):
        @pl.when(jnp.logical_or(n >= 4, not first))
        def _():
            chain(way, n, e, kind_out).wait_send()

        val = both_cores(st, n, e)
        if kind_in is not None:
            val = plus(val, kind_in, n, e)
        sbuf[way, rem(n, 4), e] = val.astype(BF16)
        chain(way, n, e, kind_out).start()

    def send_on(st, n, way, kind_in, kind_out, first, free):
        ready(st, n, free)
        for e in range(PARTS):
            send_part(st, n, e, way, kind_in, kind_out, first)

    def y_copy(n):
        k = rem(n, 2)
        return pltpu.make_async_copy(ybuf.at[k], y_ref.at[:, cols_of(n)], y_tx.at[k])

    def finish(val, n):
        @pl.when(n >= 2)
        def _():
            y_copy(n).wait()

        for e in range(PARTS):
            ybuf[rem(n, 2), :, e * hc:(e + 1) * hc] = val(e).astype(BF16)
        y_copy(n).start()

    def at(t, start, every, who):
        x = 2 * (t - start)
        n = div(x, 4) if every == 4 else div(x * 205, 1024)
        r = x - every * n
        hit = jnp.logical_and(jnp.logical_and(x >= 0, n < PIECES), r < 2)
        return n, jnp.logical_and(hit, who)

    def handoff(i):
        if i > 0:
            forwarded(block(z, i))
        if i == 2:
            for hh in range(2):
                per_way(hh, lambda cp: cp.wait_send())
        else:
            signal(fr_p.at[(0, 1, None, 2)[i]], partner)

        @pl.when(inner)
        def _():
            if i == 2:
                signal(f_in.at[1], inward)
            else:
                signal(f_in.at[(0, 1, None, 2)[i]], outward)

    def first_rows():
        own.wait()
        arrived(z)

    def again():
        @pl.when(inner)
        def _():
            signal(f_in.at[2], inward)

        @pl.when(end)
        def _():
            signal(f_out, inward)

    once = (
        (0, first_rows),
        (13, lambda: relay(1, 0)),
        (14, lambda: relay(1, 1)),
        (14, lambda: arrived(block(z, 1))),
        (16, lambda: handoff(0)),
        (25, lambda: relay(2, 0)),
        (34, lambda: relay(2, 1)),
        (36, lambda: arrived(block(z, 2))),
        (44, lambda: handoff(1)),
        (45, lambda: relay(3, 0)),
        (51, lambda: handoff(2)),
        (55, lambda: relay(3, 1)),
        (58, lambda: arrived(block(z, 3))),
        (58, again),
        (72, lambda: handoff(3)),
    )

    def step(seg, nxt, t, carry):
        lo, hi, gu, what = seg
        if gu is not None:
            @pl.when(t + 2 < hi)
            def _():
                load(t + 2, seg)

            if nxt is not None and nxt[2] is not None:
                @pl.when(t + 2 >= hi)
                def _():
                    load(t + 2, nxt)

        for when, act in once:
            if lo <= when < hi:
                pl.when(t == when)(act)

        if gu is not None:
            for cp in copies(t, seg):
                cp.wait()
        if gu:
            gate_up(t, what, t - lo)
        elif gu is False:
            st, n, seq = place(t, lo, what)

            @pl.when(seq >= 4)
            def _():
                to_partner(st, n, seq).wait_send()

            down(t, st, n, seq)

            @pl.when(t == lo)
            def _():
                pl.semaphore_wait(fr_p.at[what[0]], 1)

            to_partner(st, n, seq).start()

        def keep(n):
            from_partner(A, n)
            for e in range(PARTS):
                acc[0, n, :, e * hc:(e + 1) * hc] = plus(both_cores(A, n, e), IA, n, e)

        def last(n):
            from_partner(N, n)
            finish(lambda e: plus(both_cores(N, n, e), IN, n, e), n)

        def pieces():
            for b in range(2):
                for st, way, kind, free, g in (
                    (F, 0, IF, f_in.at[2], 2 * (t - 75) + b),
                    (N, 1, IN, f_out, 2 * (t - 75) + b - PARTS),
                ):
                    n, e = div(g, PARTS), rem(g, PARTS)

                    @pl.when(jnp.logical_and(g >= 0, g < PARTS * PIECES))
                    def _():
                        @pl.when(e == 0)
                        def _():
                            ready(st, n, free)

                        send_part(st, n, e, way, kind, IN, st == N)

        def event(start, every, who, act):
            if start >= hi or start + (every * (PIECES - 1) + 1) // 2 < lo:
                return
            n, hit = at(t, start, every, who)

            @pl.when(hit)
            def _():
                act(n)

        event(30, 4, end, lambda n: send_on(A, n, 0, None, IA, True, f_in.at[0]))
        event(34, 5, inner, keep)
        event(52, 4, end, lambda n: send_on(B, n, 0, None, IB, False, f_in.at[1]))
        event(56, 5, inner, lambda n: send_on(B, n, 0, IB, OB, True, f_in.at[1]))
        event(60, 5, inner, lambda n: finish(lambda e: plus(acc[0, n, :, e * hc:(e + 1) * hc], OB, n, e), n))
        event(73, 4, end, lambda n: send_on(F, n, 0, None, IF, False, f_in.at[2]))
        event(83, 5, end, last)
        if hi > 75:
            @pl.when(jnp.logical_and(t >= 75, inner))
            def _():
                pieces()

        return carry

    segments = segments + [(COMPUTE, LAST, None, None)]
    for seg, nxt in zip(segments, segments[1:] + [None]):
        lax.fori_loop(seg[0], seg[1], functools.partial(step, seg, nxt), 0)

    for n in (4, 5, 6, 7):
        for e in range(PARTS):
            chain(0, n, e, IN).wait_send()

        @pl.when(inner)
        def _():
            for e in range(PARTS):
                chain(1, n, e, IN).wait_send()

        to_partner(N, n, n).wait_send()
    for n in (6, 7):
        y_copy(n).wait()


def mlp(x, w_gate, w_up, w_down, vmem=67043328):
    rows, d = x.shape
    hid = w_gate.shape[1]
    dn = d // PIECES
    gn = dn // 4
    dma, reg = pltpu.SemaphoreType.DMA, pltpu.SemaphoreType.REGULAR
    return pl.pallas_call(
        kernel,
        name="mlp",
        out_shape=jax.ShapeDtypeStruct((rows, d), BF16),
        in_specs=[pl.BlockSpec(memory_space=pl.ANY)] * 4,
        out_specs=pl.BlockSpec(memory_space=pl.ANY),
        scratch_shapes=[
            pltpu.VMEM((8, rows, d), BF16),
            pltpu.VMEM((RING, 2, d, gn), BF16),
            pltpu.VMEM((3, 2, rows, hid), BF16),
            pltpu.VMEM((2 * rows, gn), F32),
            pltpu.VMEM((2 * rows, gn), F32),
            pltpu.VMEM((2, PIECES, rows, dn), F32),
            pltpu.VMEM((4, rows, dn), BF16),
            pltpu.VMEM((2, 4, PARTS, rows, dn // PARTS), BF16),
            pltpu.VMEM((2, rows, dn), BF16),
            dma((RING, 4)),
            dma,
            dma((4, 2)),
            dma((4, 2)),
            dma((4, 2)),
            dma((4, 2)),
            dma((2,)),
            dma((4, PIECES)),
            dma((5, PIECES, PARTS)),
            dma((4,)),
            dma((2, 4, PARTS)),
            dma((2,)),
            reg((3,)),
            reg((3,)),
            reg,
        ],
        compiler_params=pltpu.CompilerParams(collective_id=0, has_side_effects=True, vmem_limit_bytes=vmem),
    )(x, w_gate, w_up, w_down)


def solution(mesh):
    return jax.shard_map(
        mlp,
        mesh=mesh,
        in_specs=(P(("dp", "tp"), None), P(None, "tp"), P(None, "tp"), P("tp", None)),
        out_specs=P(("dp", "tp"), None),
        check_vma=False,
    )
```
